128 devices in a mesh: pi: 8 (over y, x_lo), pj: 16 (over x_hi, z, core).
Axes of the slice: x: 4 (x_hi: 2, x_lo: 2; x = x_hi * 2 + x_lo), y: 4, z: 4, core: 2. Of those that a mesh axis runs over, the one named last changes fastest.
Arguments:
- duo_embedding: bfloat16 [2048, 2048, 128], P('pi', 'pj'), may hold values from -12 to 12
- duo_attention_weights: float32 [128, 8], replicated, may hold values from -16 to 16
- aligned_embedding: bfloat16 [512, 64, 2048], P('pj', None, 'pi'), may hold values from -6 to 6
- aligned_scaling_weights: float32 [64], replicated, may hold values from 0.5 to 1.5
- aligned_shift_vector: float32 [64], replicated, may hold values from -3 to 3
- payload_weights: bfloat16 [64, 256], replicated, may hold values from -0.75 to 0.75
- switch_weights: bfloat16 [64, 256], replicated, may hold values from -0.75 to 0.75
- closing_weights: bfloat16 [256, 64], replicated, may hold values from -1.5 to 1.5
Outputs:
- update: bfloat16 [512, 64, 2048], P('pj', None, 'pi')
The draws below stay inside these ranges and needn't reach their ends.
All inputs are finite; a program needn't handle non-finite values.
Results may differ from the reference program's by a relative error of at most 0.009.
Values may be sent and summed in bfloat16 or wider, within the bound.
No kernel may reach another device: no remote copies, remote signals or barrier semaphores. Data moves between devices by JAX's collectives and lax.ppermute only.
A program may use at most 192 MiB of HBM per device.

```python
import math
import jax
import jax.numpy as jnp
from jax import lax

ALIGNED_EMBED = 64
CZ = 128
ATTENDER_TALLY = 8
UNIT_SPAN = 32
POSITION_TALLY = 2048
ALIGNED_SEQS = 512
JOINT_SPAN = 256


def head_directions(key):
    random_dirs = jax.random.normal(jax.random.fold_in(key, 7001), (ATTENDER_TALLY, CZ), jnp.float32)
    random_dirs = random_dirs - jnp.mean(random_dirs, axis=1, keepdims=True)
    return random_dirs / jnp.sqrt(jnp.sum(random_dirs * random_dirs, axis=1, keepdims=True))


def score_weights(key):
    directions = head_directions(key)
    noise = jnp.clip(jax.random.normal(jax.random.fold_in(key, 7002), (CZ, ATTENDER_TALLY), jnp.float32), -6.0, 6.0)
    return 0.18 * noise + 0.35 * directions.T


def draw_duo_attention_weights(key, part):
    return score_weights(key)


def draw_duo_embedding(key, part):
    directions = head_directions(key)
    noise = jnp.clip(jax.random.normal(jax.random.fold_in(key, 7003), (POSITION_TALLY, POSITION_TALLY, CZ), jnp.float32), -6.0, 6.0)
    column_ramp = 2.0 * (2.0 * jnp.arange(POSITION_TALLY, dtype=jnp.float32) / (POSITION_TALLY - 1) - 1.0)
    pair_field = noise + column_ramp[None, :, None] * jnp.sum(directions, axis=0)[None, None, :]
    return pair_field.astype(jnp.bfloat16)


def level_of(key, extent, shards, least, high):
    loudness = 1.0
    for position, blocks in shards:
        heights = jax.random.uniform(jax.random.fold_in(jax.random.fold_in(key, 6), position), (blocks,), jnp.float32, least / len(shards), high / len(shards))
        loudness = loudness * jnp.repeat(jnp.exp(heights), extent[position] // blocks).reshape((-1,) + (1,) * (len(extent) - 1 - position))
    return loudness


def scatter_about(stream_key, extent, width, reach, cuts=(), kind=jnp.bfloat16):
    factor_of = level_of(stream_key, extent, cuts, -0.22, 0.18) if cuts else 1.0
    array = jax.random.normal(stream_key, extent, jnp.float32) * width * factor_of
    return jnp.minimum(jnp.maximum(array, -reach), reach).astype(kind)


def setup_inputs(seed: int = 0) -> dict:
    streams_of = jax.random.split(jax.random.key(seed), 9)
    return {
        "duo_embedding": draw_duo_embedding(jax.random.fold_in(streams_of[8], 71), 0),
        "duo_attention_weights": draw_duo_attention_weights(jax.random.fold_in(streams_of[8], 71), 0),
        "aligned_embedding": scatter_about(streams_of[2], (ALIGNED_SEQS, ALIGNED_EMBED, POSITION_TALLY), 1.0, 6.0, ((0, 16), (2, 8))),
        "aligned_scaling_weights": jnp.clip(1.0 + 0.1 * jax.random.normal(streams_of[3], (ALIGNED_EMBED,), jnp.float32), 0.5, 1.5),
        "aligned_shift_vector": scatter_about(streams_of[4], (ALIGNED_EMBED,), 0.5, 3.0, (), jnp.float32),
        "payload_weights": scatter_about(streams_of[5], (ALIGNED_EMBED, JOINT_SPAN), ALIGNED_EMBED ** -0.5, 0.75),
        "switch_weights": scatter_about(streams_of[6], (ALIGNED_EMBED, JOINT_SPAN), ALIGNED_EMBED ** -0.5, 0.75),
        "closing_weights": scatter_about(streams_of[7], (JOINT_SPAN, ALIGNED_EMBED), (JOINT_SPAN // 16) ** -0.5, 1.5),
    }


EPS = 1e-05

def rescale_embedding(inputs, axis):
    row_mean = lax.optimization_barrier(jnp.mean(inputs, axis=axis, keepdims=True))
    centred = inputs - row_mean
    variance = lax.optimization_barrier(jnp.mean(centred * centred, axis=axis, keepdims=True))
    return centred * lax.rsqrt(variance + EPS)

def reference(duo_embedding, duo_attention_weights, aligned_embedding, aligned_scaling_weights, aligned_shift_vector, payload_weights, switch_weights, closing_weights):
    aligned_fullbit_copy = aligned_embedding.astype(jnp.float32)
    rescaled_aligned = (rescale_embedding(aligned_fullbit_copy, 1) * aligned_scaling_weights[None, :, None] + aligned_shift_vector[None, :, None]).astype(jnp.bfloat16)
    normed_float = rescaled_aligned.astype(jnp.float32)
    payloads = jnp.einsum('scn,ce->sen', normed_float, payload_weights.astype(jnp.float32)).astype(jnp.bfloat16)
    switch_share = jax.nn.sigmoid(jnp.einsum('scn,ce->sen', normed_float, switch_weights.astype(jnp.float32)))
    payload_each_attender = payloads.astype(jnp.float32).reshape(ALIGNED_SEQS, ATTENDER_TALLY, UNIT_SPAN, POSITION_TALLY)
    tile_entries = math.gcd(POSITION_TALLY, 256)
    block_count = POSITION_TALLY // tile_entries

    def one_block(block_index):
        start_position = (block_index * tile_entries).astype(jnp.int32)
        pair_tile = lax.dynamic_slice_in_dim(duo_embedding, start_position, tile_entries, 0).astype(jnp.float32)
        pair_normed = rescale_embedding(pair_tile, 2)
        scores = jnp.einsum('ijc,ch->hij', pair_normed, duo_attention_weights, precision=lax.Precision.HIGHEST)
        row_peak = lax.optimization_barrier(jnp.max(scores, axis=2, keepdims=True))
        exp_scores = jnp.exp(scores - row_peak).astype(jnp.bfloat16)
        exp_float = exp_scores.astype(jnp.float32)
        row_total = lax.optimization_barrier(jnp.sum(exp_float, axis=2))
        numerator = jnp.einsum('hij,shcj->shci', exp_float, payload_each_attender)
        switch_tile = lax.dynamic_slice_in_dim(switch_share, start_position, tile_entries, 2).reshape(ALIGNED_SEQS, ATTENDER_TALLY, UNIT_SPAN, tile_entries)
        averaged_result = (switch_tile * (numerator / row_total[None, :, None, :])).astype(jnp.bfloat16)
        averaged_result = averaged_result.reshape(ALIGNED_SEQS, ATTENDER_TALLY * UNIT_SPAN, tile_entries).astype(jnp.float32)
        return jnp.einsum('ser,ec->scr', averaged_result, closing_weights.astype(jnp.float32)).astype(jnp.bfloat16)
    result_tiles = lax.map(one_block, jnp.arange(block_count, dtype=jnp.int32))
    return jnp.transpose(result_tiles, (1, 2, 0, 3)).reshape(ALIGNED_SEQS, ALIGNED_EMBED, POSITION_TALLY)
```

```python
import math
import jax
import jax.numpy as jnp
from jax import lax
from jax.experimental import pallas as pl
from jax.experimental.pallas import tpu as pltpu
from jax.sharding import Mesh
from jax.sharding import PartitionSpec as P

PI = ("y", "xl")
PJ = ("xh", "z", "c")
EPS = 1e-05
LOG2E = math.log2(math.e)
F32 = jnp.float32
BF16 = jnp.bfloat16


NT = (((1,), (1,)), ((), ()))


def score_kernel(x_ref, w_ref, out_ref, t_ref):
    step = pl.program_id(0)
    rows = x_ref.shape[0]
    heads = w_ref.shape[0]
    total = t_ref.shape[0] // heads
    cols = x_ref.shape[1]
    cz = x_ref.shape[2]
    w = w_ref[...]
    wc = (w - jnp.mean(w, axis=1, keepdims=True)) * LOG2E
    hi = wc.astype(BF16).astype(F32)
    rest = wc - hi
    mid = rest.astype(BF16).astype(F32)
    low = rest - mid
    lhs = jnp.concatenate([hi, mid, low, jnp.zeros_like(low)], axis=0).astype(BF16)
    ones = jnp.ones((16, cz), BF16)

    for i in range(0, rows, 2):
        x = x_ref[i : i + 2].reshape(2 * cols, cz)
        xf = x.astype(F32)
        d = xf - jnp.sum(xf, axis=1, keepdims=True) * (1.0 / cz)
        sq = d * d
        sq_hi = sq.astype(BF16)
        sq_lo = (sq - sq_hi.astype(F32)).astype(BF16)
        var = lax.dot_general(ones, sq_hi, NT, preferred_element_type=F32) + lax.dot_general(
            ones, sq_lo, NT, preferred_element_type=F32
        )
        s = lax.dot_general(lhs, x, NT, preferred_element_type=F32)
        t = (s[0:8] + s[8:16] + s[16:24]) * lax.rsqrt(var[0:8] * (1.0 / cz) + EPS)
        at = pl.multiple_of((step * rows + i) * heads, 2 * heads)
        t_ref[pl.ds(at, heads), :] = t[:, :cols]
        t_ref[pl.ds(at + heads, heads), :] = t[:, cols:]

    @pl.when(step == pl.num_programs(0) - 1)
    def _():
        peaks = []
        for h in range(heads):
            t = t_ref[pl.ds(h, total, stride=heads), :].T
            peak = jnp.max(t, axis=0, keepdims=True)
            peak = jnp.round(peak).astype(BF16).astype(F32)
            out_ref[h * cols : (h + 1) * cols, :] = jnp.exp2(t - peak).astype(BF16)
            peaks.append(peak)
        peaks = jnp.concatenate(peaks + [jnp.zeros((heads, total), F32)], axis=0)
        out_ref[heads * cols :, :] = peaks.astype(BF16)


def pair_scores(pair, w):
    rows, cols, cz = pair.shape
    heads = w.shape[1]
    step = 16
    return pl.pallas_call(
        score_kernel,
        out_shape=jax.ShapeDtypeStruct((heads * cols + 16, rows), BF16),
        grid=(rows // step,),
        in_specs=[
            pl.BlockSpec((step, cols, cz), lambda i: (i, 0, 0)),
            pl.BlockSpec((heads, cz), lambda i: (0, 0)),
        ],
        out_specs=pl.BlockSpec((heads * cols + 16, rows), lambda i: (0, 0)),
        scratch_shapes=[pltpu.VMEM((rows * heads, cols), F32)],
        compiler_params=pltpu.CompilerParams(vmem_limit_bytes=24 << 20),
        cost_estimate=pl.CostEstimate(
            flops=20_000_000_000, bytes_accessed=pair.size * 2, transcendentals=0
        ),
        name="pair_scores",
    )(pair, w.T)


def rescale(x, gain, bias):
    mean = jnp.mean(x, axis=0, keepdims=True)
    centred = x - mean
    var = jnp.mean(centred * centred, axis=0, keepdims=True)
    return (centred * lax.rsqrt(var + EPS) * gain + bias).astype(BF16)


CHUNK = 8


def mix_kernel(
    where_ref, gain_ref, bias_ref, pay_ref, switch_ref, close_ref, *refs
):
    xs, ws = refs[:10], refs[10:26]
    out_ref = refs[26]
    xv, wv, kv, vv, tot, wo, xsem, wsem, ksem = refs[27:]
    heads, tokens, rows = wv.shape
    seqs, chans, span = xs[0].shape
    cols = tokens // 16
    half = seqs // 2
    ex = heads * 32

    def x_copies(chunk):
        lo = chunk * CHUNK
        made = []
        for slot in range(6):
            made.append((xs[slot], slot, lo))
        made.append((xs[6 if lo < half else 7], 6, lo % half))
        made.append((xs[8 if lo < half else 9], 7, lo % half))
        return [
            pltpu.make_async_copy(
                src.at[pl.ds(at, CHUNK)],
                xv.at[where_ref[slot], pl.ds(lo, CHUNK)],
                xsem.at[chunk, slot],
            )
            for src, slot, at in made
        ]

    def w_copies(b):
        at = where_ref[8 + b]
        made = [
            pltpu.make_async_copy(
                ws[b].at[pl.ds(h * cols, cols)],
                wv.at[h, pl.ds(pl.multiple_of(at * cols, cols), cols)],
                wsem.at[b, h],
            )
            for h in range(heads)
        ]
        made.append(
            pltpu.make_async_copy(ws[b].at[pl.ds(heads * cols, 16)], kv.at[b], ksem.at[b])
        )
        return made

    for c in x_copies(0):
        c.start()
    for b in range(16):
        for c in w_copies(b):
            c.start()
    for chunk in range(1, seqs // CHUNK):
        for c in x_copies(chunk):
            c.start()

    gain = gain_ref[...]
    bias = bias_ref[...]
    pay = pay_ref[...]

    for chunk in range(seqs // CHUNK):
        for c in x_copies(chunk):
            c.wait()

        def values(s, _):
            for n in range(8):
                x = xv[n, chunk * CHUNK + s].astype(F32)
                normed = rescale(x, gain, bias)
                v = jnp.dot(pay, normed, preferred_element_type=F32).astype(BF16)
                for h in range(heads):
                    vv[h, pl.ds(pl.multiple_of(s * 32, 32), 32), n * span : (n + 1) * span] = v[
                        h * 32 : (h + 1) * 32
                    ]
            return 0

        lax.fori_loop(0, CHUNK, values, 0)

        if chunk == 0:
            for b in range(16):
                for c in w_copies(b):
                    c.wait()
            peak = kv[0].astype(F32)
            for b in range(1, 16):
                peak = jnp.maximum(peak, kv[b].astype(F32))
            kv2 = [jnp.exp2(kv[b].astype(F32) - peak) for b in range(16)]
            for h in range(heads):
                acc = jnp.zeros((8, rows), F32)
                for b in range(16):
                    at = pl.ds(pl.multiple_of(where_ref[8 + b] * cols, cols), cols)
                    w = wv[h, at].astype(F32) * kv2[b][h : h + 1]
                    wv[h, at] = w.astype(BF16)
                    acc = acc + jnp.sum(w.reshape(cols // 8, 8, rows), axis=0)
                tot[h : h + 1] = 1.0 / jnp.sum(acc, axis=0, keepdims=True)

        def gates(s, _):
            x = xv[where_ref[0], chunk * CHUNK + s].astype(F32)
            normed = rescale(x, gain, bias)
            g = jnp.dot(switch_ref[...], normed, preferred_element_type=F32)
            g = 0.5 * jnp.tanh(0.5 * g) + 0.5
            for h in range(heads):
                wo[h, pl.ds(pl.multiple_of(s * 32, 32), 32)] = g[h * 32 : (h + 1) * 32]
            return 0

        lax.fori_loop(0, CHUNK, gates, 0)

        def attend(h, _):
            num = jnp.dot(vv[h], wv[h], preferred_element_type=F32)
            wo[h] = wo[h] * (num * tot[pl.ds(h, 1)])
            return 0

        lax.fori_loop(0, heads, attend, 0)

        def close(s, _):
            at = pl.ds(pl.multiple_of(s * 32, 32), 32)
            w = jnp.concatenate([wo[h, at] for h in range(heads)], axis=0).astype(BF16)
            out_ref[chunk * CHUNK + s] = jnp.dot(
                close_ref[...], w, preferred_element_type=F32
            ).astype(BF16)
            return 0

        lax.fori_loop(0, CHUNK, close, 0)


def mix(where, gain, bias, pay, switch, close, xs, ws):
    seqs, chans, span = xs[0].shape
    rows = ws[0].shape[1]
    heads = 8
    cols = (ws[0].shape[0] - 16) // heads
    tokens = 16 * cols
    vm = pl.BlockSpec(memory_space=pltpu.VMEM)
    anyspec = pl.BlockSpec(memory_space=pl.ANY)
    return pl.pallas_call(
        mix_kernel,
        out_shape=jax.ShapeDtypeStruct((seqs, chans, rows), BF16),
        in_specs=[pl.BlockSpec(memory_space=pltpu.SMEM)] + [vm] * 5 + [anyspec] * 26,
        out_specs=vm,
        scratch_shapes=[
            pltpu.VMEM((8, seqs, chans, span), BF16),
            pltpu.VMEM((heads, tokens, rows), BF16),
            pltpu.VMEM((16, 16, rows), BF16),
            pltpu.VMEM((heads, CHUNK * 32, tokens), BF16),
            pltpu.VMEM((heads, rows), F32),
            pltpu.VMEM((heads, CHUNK * 32, rows), F32),
            pltpu.SemaphoreType.DMA((seqs // CHUNK, 8)),
            pltpu.SemaphoreType.DMA((16, heads)),
            pltpu.SemaphoreType.DMA((16,)),
        ],
        compiler_params=pltpu.CompilerParams(vmem_limit_bytes=56 << 20),
        cost_estimate=pl.CostEstimate(
            flops=20_000_000_000, bytes_accessed=18 << 20, transcendentals=0
        ),
        name="mix",
    )(where, gain, bias, pay, switch, close, *xs, *ws)


def shift(x, axis, by, size):
    return lax.ppermute(x, axis, [(i, (i + by) % size) for i in range(size)])


def body(pair, pair_w, x0, gain, bias, pay, switch, close):
    xp = shift(x0, "xl", 1, 2)
    xu = shift(x0, "y", 1, 4)
    xd = shift(x0, "y", -1, 4)
    half = x0.shape[0] // 2
    xou = shift(xu[:half], "y", 1, 4)
    xod = shift(xd[half:], "y", -1, 4)
    xpu = shift(xp, "y", 1, 4)
    xpd = shift(xp, "y", -1, 4)
    xpou = shift(xou, "xl", 1, 2)
    xpod = shift(xod, "xl", 1, 2)

    w0 = pair_scores(pair, pair_w)
    wu = shift(w0, "z", 1, 4)
    wd = shift(w0, "z", -1, 4)
    wx = shift(w0, "xh", 1, 2)
    wxu = shift(wx, "z", 1, 4)
    wxd = shift(wx, "z", -1, 4)
    wo = shift(wu, "z", 1, 4)
    wxo = shift(wxd, "z", -1, 4)
    mine = [w0, wu, wd, wx, wxu, wxd, wo, wxo]
    other = [shift(w, "c", 1, 2) for w in mine]

    y, xl, xh, z, c = (lax.axis_index(a) for a in ("y", "xl", "xh", "z", "c"))
    block = lambda dy, dx: ((y + dy) % 4) * 2 + (xl + dx) % 2
    spot = lambda dx, dz, dc: ((xh + dx) % 2) * 8 + ((z + dz) % 4) * 2 + (c + dc) % 2
    moves = [(0, 0), (0, -1 % 4), (0, 1), (1, 0), (1, -1 % 4), (1, 1), (0, 2), (1, 2)]
    where = jnp.stack(
        [block(0, 0), block(0, 1), block(3, 0), block(1, 0), block(3, 1), block(1, 1), block(2, 0), block(2, 1)]
        + [spot(dx, dz, 0) for dx, dz in moves]
        + [spot(dx, dz, 1) for dx, dz in moves]
    ).astype(jnp.int32)
    wide = lambda v: jnp.broadcast_to(v[:, None], (v.shape[0], x0.shape[2]))
    return mix(
        where, wide(gain), wide(bias), pay.T, switch.T, close.T,
        [x0, xp, xu, xd, xpu, xpd, xou, xod, xpou, xpod], mine + other,
    )


def solution(mesh):
    finer = Mesh(mesh.devices.reshape(4, 2, 2, 4, 2), PI + PJ)
    placed = (P(PI, PJ, None), P(), P(PJ, None, PI), P(), P(), P(), P(), P())
    return jax.shard_map(
        body, mesh=finer, in_specs=placed, out_specs=P(PJ, None, PI), check_vma=False
    )
```
